32 devices in a mesh: ty: 4 (over y, x), tx: 8 (over z, core).
Axes of the slice: x: 2, y: 2, z: 4, core: 2. Of those that a mesh axis runs over, the one named last changes fastest.
Arguments:
- object_slices: float32 [2, 2, 1024, 2048], P(None, None, 'ty', 'tx'), may hold values from -5 to 5
- probe: float32 [2, 256, 256], replicated, may hold values from -5 to 5
- position_count: int32 [4, 8], P('ty', 'tx'), may hold values from 1 to 5, as said below
- offsets: int32 [4, 8, 5, 2], P('ty', 'tx'), may hold values from 0 to 128
- intensities: float32 [4, 8, 5, 256, 256], P('ty', 'tx'), may hold values from 0 to 2
Outputs:
- object_new: float32 [2, 2, 1024, 2048], P(None, None, 'ty', 'tx')
- probe_new: float32 [2, 256, 256], replicated
The draws below stay inside these ranges and needn't reach their ends.
Inputs may be any that keep to these rules, and one draw needn't show every extreme that they name: `position_count`: each tile has 1 to 5 positions; some tile has exactly 5.
All inputs are finite; a program needn't handle non-finite values.
Results may differ from the reference program's by a relative error of at most 0.0003.
Values sent between devices are 32-bit elements; how exact they have to be, the bound alone decides.
No kernel may reach another device: no remote copies, remote signals or barrier semaphores. Data moves between devices by JAX's collectives and lax.ppermute only.
A program may use at most 128 MiB of HBM per device.

```python
import math
import jax
import jax.numpy as jnp
from jax import lax

PROBE = 256
CORE = 256
MARGIN = 64
MAXPOS = 5
ITERS = 2
NY = 1024
NX = 2048
N_TY = 4
N_TX = 8


def draw_position_count(key, part):
    first = jax.random.fold_in(key, 11)
    second = jax.random.fold_in(key, 23)
    counts = jax.random.randint(first, (N_TY * N_TX,), 1, MAXPOS + 1)
    chosen = jax.random.randint(second, (), 0, N_TY * N_TX)
    counts = counts.at[chosen].set(MAXPOS)
    return counts.reshape(N_TY, N_TX).astype(jnp.int32)


def set_ends(drawn, key, low, top_value):
    dims = drawn.shape
    index_at = [jax.random.randint(jax.random.fold_in(key, axis), (), 0, dims[axis]) for axis in range(len(dims))]
    drawn = drawn.at[tuple(index_at)].set(low)
    longest = dims.index(max(dims))
    index_at[longest] = (index_at[longest] + 1) % dims[longest]
    return drawn.at[tuple(index_at)].set(top_value)


def block_scale(key, shape, cuts, smallest, high):
    gain = 1.0
    for dim, blocks in cuts:
        heights = jax.random.uniform(jax.random.fold_in(jax.random.fold_in(key, 6), dim), (blocks,), jnp.float32, smallest / len(cuts), high / len(cuts))
        gain = gain * jnp.repeat(jnp.exp(heights), shape[dim] // blocks).reshape((-1,) + (1,) * (len(shape) - 1 - dim))
    return gain


def gaussian(stream_key, shape, deviation, reach, shards=(), kind=jnp.bfloat16):
    factor_of = block_scale(stream_key, shape, shards, -0.22, 0.18) if shards else 1.0
    array = jax.random.normal(stream_key, shape, jnp.float32) * deviation * factor_of
    return jnp.minimum(jnp.maximum(array, -reach), reach).astype(kind)


def setup_inputs(seed: int = 0) -> dict:
    key_list = jax.random.split(jax.random.key(seed), 6)
    object_slices = gaussian(key_list[0], (2, 2, NY, NX), 0.7, 5.0, ((2, 4), (3, 8)), jnp.float32)
    probe = gaussian(key_list[1], (2, PROBE, PROBE), 0.7, 5.0, (), jnp.float32)
    position_count = draw_position_count(jax.random.fold_in(key_list[5], 71), 0)
    offsets = set_ends(jax.random.randint(key_list[3], (N_TY, N_TX, MAXPOS, 2), 0, CORE + 2 * MARGIN - PROBE + 1), jax.random.fold_in(key_list[3], 1), 0, CORE + 2 * MARGIN - PROBE).astype(jnp.int32)
    intensities = jnp.clip(2.0 * jax.random.uniform(key_list[4], (N_TY, N_TX, MAXPOS, PROBE, PROBE), jnp.float32) ** block_scale(key_list[4], (N_TY, N_TX, MAXPOS, PROBE, PROBE), ((0, 4), (1, 8)), -0.2, 0.2), 0.0, 2.0)
    return dict(object_slices=object_slices, probe=probe, position_count=position_count, offsets=offsets, intensities=intensities)


chirp_rate = 0.5
object_rate = 0.5
probe_rate = 2.0

def matmul(left, right):
    return jnp.dot(left, right, precision=lax.Precision.HIGHEST, preferred_element_type=jnp.float32)

def complex_product(left_real, left_imag, right_real, right_imag):
    out_real = matmul(left_real, right_real) - matmul(left_imag, right_imag)
    out_imag = matmul(left_real, right_imag) + matmul(left_imag, right_real)
    return (out_real, out_imag)

def dft_tables(size):
    index = lax.iota(jnp.int32, size)
    product = index[:, None] * index[None, :] % size
    angles = product.astype(jnp.float32) * (2.0 * math.pi / size)
    factor = 1.0 / math.sqrt(size)
    four_real = jnp.cos(angles) * factor
    four_imag = -jnp.sin(angles) * factor
    centred = ((index + size // 2) % size - size // 2).astype(jnp.float32)
    phases = centred * centred * (chirp_rate * math.pi / size)
    kernel_real = jnp.cos(phases)
    kernel_imag = -jnp.sin(phases)
    scaled_real = four_real * kernel_real[None, :] + four_imag * kernel_imag[None, :]
    scaled_imag = four_real * kernel_imag[None, :] - four_imag * kernel_real[None, :]
    prop_real, prop_imag = complex_product(scaled_real, scaled_imag, four_real, four_imag)
    return (four_real, four_imag, prop_real, prop_imag)

def forward_pair(mat_real, mat_imag, field_real, field_imag):
    mid_real, mid_imag = complex_product(mat_real, mat_imag, field_real, field_imag)
    return complex_product(mid_real, mid_imag, mat_real.T, mat_imag.T)

def adjoint_pair(mat_real, mat_imag, field_real, field_imag):
    mid_real, mid_imag = complex_product(mat_real.T, -mat_imag.T, field_real, field_imag)
    return complex_product(mid_real, mid_imag, mat_real, -mat_imag)

def position_grad(probe_now, window, measured, tables):
    four_real, four_imag, prop_real, prop_imag = tables
    probe_real, probe_imag = (probe_now[0], probe_now[1])
    one_real, one_imag, two_real, two_imag = (window[0], window[1], window[2], window[3])
    wave_real = probe_real * one_real - probe_imag * one_imag
    wave_imag = probe_real * one_imag + probe_imag * one_real
    moved_real, moved_imag = forward_pair(prop_real, prop_imag, wave_real, wave_imag)
    exit_real = moved_real * two_real - moved_imag * two_imag
    exit_imag = moved_real * two_imag + moved_imag * two_real
    far_real, far_imag = forward_pair(four_real, four_imag, exit_real, exit_imag)
    misfit = far_real * far_real + far_imag * far_imag - measured
    back_real, back_imag = adjoint_pair(four_real, four_imag, misfit * far_real, misfit * far_imag)
    grad_two_real = moved_real * back_real + moved_imag * back_imag
    grad_two_imag = moved_real * back_imag - moved_imag * back_real
    gmove_real = two_real * back_real + two_imag * back_imag
    gmove_imag = two_real * back_imag - two_imag * back_real
    gwave_real, gwave_imag = adjoint_pair(prop_real, prop_imag, gmove_real, gmove_imag)
    grad_one_real = probe_real * gwave_real + probe_imag * gwave_imag
    grad_one_imag = probe_real * gwave_imag - probe_imag * gwave_real
    gprobe_real = one_real * gwave_real + one_imag * gwave_imag
    gprobe_imag = one_real * gwave_imag - one_imag * gwave_real
    object_part = jnp.stack([grad_one_real, grad_one_imag, grad_two_real, grad_two_imag])
    return (object_part, jnp.stack([gprobe_real, gprobe_imag]))

def reference(object_slices, probe, position_count, offsets, intensities):
    tables = dft_tables(PROBE)
    extent = CORE + 2 * MARGIN
    objects = object_slices.reshape(4, NY, NX)
    probe_now = probe
    zero = jnp.int32(0)
    for step in range(ITERS):
        padded = jnp.pad(objects, ((0, 0), (MARGIN, MARGIN), (MARGIN, MARGIN)), mode='wrap')

        def tile(index, carry):
            grads, probe_grad = carry
            row = (index // N_TX).astype(jnp.int32)
            column = (index % N_TX).astype(jnp.int32)
            extended = lax.dynamic_slice(padded, (zero, row * CORE, column * CORE), (4, extent, extent))

            def visit(slot, inner):
                local, local_probe = inner
                top = offsets[row, column, slot, 0].astype(jnp.int32)
                left = offsets[row, column, slot, 1].astype(jnp.int32)
                window = lax.dynamic_slice(extended, (zero, top, left), (4, PROBE, PROBE))
                object_part, probe_part = position_grad(probe_now, window, intensities[row, column, slot], tables)
                current = lax.dynamic_slice(local, (zero, top, left), (4, PROBE, PROBE))
                local = lax.dynamic_update_slice(local, current + object_part, (zero, top, left))
                return (local, local_probe + probe_part)
            start = (jnp.zeros((4, extent, extent), jnp.float32), jnp.zeros((2, PROBE, PROBE), jnp.float32))
            local, local_probe = lax.fori_loop(zero, position_count[row, column].astype(jnp.int32), visit, start)
            current = lax.dynamic_slice(grads, (zero, row * CORE, column * CORE), (4, extent, extent))
            grads = lax.dynamic_update_slice(grads, current + local, (zero, row * CORE, column * CORE))
            return (grads, probe_grad + local_probe)
        begin = (jnp.zeros((4, NY + 2 * MARGIN, NX + 2 * MARGIN), jnp.float32), jnp.zeros((2, PROBE, PROBE), jnp.float32))
        grads, probe_grad = lax.fori_loop(0, N_TY * N_TX, tile, begin)
        rows = grads[:, MARGIN:MARGIN + NY, :]
        rows = rows.at[:, NY - MARGIN:, :].add(grads[:, :MARGIN, :])
        rows = rows.at[:, :MARGIN, :].add(grads[:, NY + MARGIN:, :])
        total = rows[:, :, MARGIN:MARGIN + NX]
        total = total.at[:, :, NX - MARGIN:].add(rows[:, :, :MARGIN])
        total = total.at[:, :, :MARGIN].add(rows[:, :, NX + MARGIN:])
        peak = jnp.max(probe_now[0] * probe_now[0] + probe_now[1] * probe_now[1]) + 1e-06
        objects = objects - object_rate / peak * total
        probe_now = probe_now - probe_rate / (N_TY * N_TX) * probe_grad
    return (objects.reshape(2, 2, NY, NX), probe_now)
```

```python
import math

import jax
import jax.numpy as jnp
import ml_dtypes
import numpy as np
from jax import lax
from jax.experimental import pallas as pl
from jax.experimental.pallas import tpu as pltpu
from jax.sharding import PartitionSpec as P

MARGIN = 64
ITERS = 2
CHUNK = 16

chirp_rate = 0.5
object_rate = 0.5
probe_rate = 2.0


def tables(size):
    index = np.arange(size)
    four = np.exp(-2j * np.pi * (np.outer(index, index) % size) / size) / math.sqrt(size)
    centred = (index + size // 2) % size - size // 2
    kernel = np.exp(-1j * chirp_rate * np.pi * centred * centred / size)
    prop = (four.conj() * kernel[None, :]) @ four
    half = size // 2
    near, far = prop[:half, :half], prop[:half, half:]
    blocks = ((0.5 * (near + far), 0.5 * (near - far)), (four[0::2, :half], four[1::2, :half]))
    out = np.zeros((2, 2, 2, 2, size, size), ml_dtypes.bfloat16)
    for family in range(2):
        for parity in range(2):
            block = blocks[family][parity]
            left = np.block([[block.real, -block.imag], [block.imag, block.real]])
            for form, value in enumerate((left, left.T)):
                high = value.astype(np.float32).astype(ml_dtypes.bfloat16)
                low = (value - high.astype(np.float64)).astype(np.float32).astype(ml_dtypes.bfloat16)
                out[family, parity, form, 0] = high
                out[family, parity, form, 1] = low
    return out


def lane_order(size):
    out = np.zeros((size, size), ml_dtypes.bfloat16)
    half = size // 2
    for lane in range(half):
        out[2 * lane, lane] = 1
        out[2 * lane + 1, half + lane] = 1
    return np.stack([out, out.T])


def dot(left, right):
    return jnp.dot(left, right, preferred_element_type=jnp.float32)


def parts(value):
    high = value.astype(jnp.bfloat16)
    low = (value - high.astype(jnp.float32)).astype(jnp.bfloat16)
    return high, low


def thirds(value):
    first = value.astype(jnp.bfloat16)
    rest = value - first.astype(jnp.float32)
    second = rest.astype(jnp.bfloat16)
    return first, second, (rest - second.astype(jnp.float32)).astype(jnp.bfloat16)


def sort_kernel(count_ref, values_ref, order_ref, out_ref):
    out_ref[...] = jnp.zeros_like(out_ref)

    def visit(slot, carry):
        first, second, third = [dot(x, order_ref[0]) for x in thirds(values_ref[slot])]
        first, second, third = [dot(order_ref[1], x) for x in thirds((first + second) + third)]
        out_ref[slot] = (first + second) + third
        return carry

    lax.fori_loop(0, count_ref[0], visit, 0)


def grad_kernel(
    count_ref, offset_ref, core_ref, row_ref, col_ref, corner_ref, probe_ref, measured_ref, table_ref,
    gcore_ref, grow_ref, gcol_ref, gcorner_ref, gprobe_ref,
    window_ref, moved_ref, rolled_ref, high_ref, low_ref, rhigh_ref, rlow_ref, mid_ref, back_ref,
):
    size = probe_ref.shape[1]
    half = size // 2
    quarter = size // 4
    lane = lax.broadcasted_iota(jnp.int32, (CHUNK, half), 1)
    row = lax.broadcasted_iota(jnp.int32, (CHUNK, half), 0)
    for ref in (gcore_ref, grow_ref, gcol_ref, gcorner_ref, gprobe_ref):
        ref[...] = jnp.zeros_like(ref)

    def at(part, start):
        return pl.ds(part * half + start, CHUNK)

    def lanes(part):
        return pl.ds(part * half, half)

    def fold(quads):
        mixed = [[quads[0][c] + quads[1][c] for c in range(2)], [quads[0][c] - quads[1][c] for c in range(2)]]
        return [[m[0] + m[1], m[0] - m[1]] for m in mixed]

    def put_right(start, real, imag):
        for p in range(2):
            for q in range(2):
                for comp, value in ((0, real[p][q]), (1, imag[p][q])):
                    high, low = parts(value)
                    high_ref[q, at(p, start), lanes(comp)] = high
                    low_ref[q, at(p, start), lanes(comp)] = low

    def right(family, form):
        for q in range(2):
            weight, small = table_ref[family, q, form, 0], table_ref[family, q, form, 1]
            mid_ref[q] = dot(high_ref[q], weight) + dot(low_ref[q], weight) + dot(high_ref[q], small)

    def left(family, form):
        for q in range(2):
            for p in range(2):
                for start in range(0, half, CHUNK):
                    for comp in range(2):
                        high, low = parts(mid_ref[q, at(p, start), lanes(comp)])
                        rhigh_ref[p, at(comp, start), lanes(q)] = high
                        rlow_ref[p, at(comp, start), lanes(q)] = low
        for p in range(2):
            weight, small = table_ref[family, p, form, 0], table_ref[family, p, form, 1]
            back_ref[p] = dot(weight, rhigh_ref[p]) + dot(small, rhigh_ref[p]) + dot(weight, rlow_ref[p])

    def take(start, comp):
        return [[back_ref[p, at(comp, start), lanes(q)] for q in range(2)] for p in range(2)]

    def visit(slot, carry):
        top = offset_ref[slot, 0]
        lead = offset_ref[slot, 1]
        shift_row = lax.rem(top + (size - MARGIN), size)
        shift_col = lax.rem(lead + (size - MARGIN), size)
        for comp in range(2):
            rolled_ref[comp] = pltpu.roll(pltpu.roll(probe_ref[comp], shift_row, 0), shift_col, 1)
        cols = (lane + MARGIN >= lead, lane - MARGIN < lead)

        def row_mask(part, start):
            inside = row + start
            return inside + MARGIN >= top if part == 0 else inside - MARGIN < top

        def boundary(part, start):
            return (start < quarter) == (part == 0)

        for start in range(0, half, CHUNK):
            one = [[None, None], [None, None]]
            for r in range(2):
                edge = boundary(r, start)
                mask = row_mask(r, start) if edge else None
                for c in range(2):
                    values = []
                    for k in range(4):
                        own = core_ref[k, at(r, start), lanes(c)]
                        other = col_ref[k, at(r, start), :]
                        if edge:
                            own = jnp.where(mask, own, row_ref[k, pl.ds(start, CHUNK), lanes(c)])
                            other = jnp.where(mask, other, corner_ref[k, pl.ds(start, CHUNK), :])
                        value = jnp.where(cols[c], own, other)
                        window_ref[k, at(r, start), lanes(c)] = value
                        values.append(value)
                    pr, pi = rolled_ref[0, at(r, start), lanes(c)], rolled_ref[1, at(r, start), lanes(c)]
                    one[r][c] = (pr * values[0] - pi * values[1], pr * values[1] + pi * values[0])
            real = fold([[one[r][c][0] for c in range(2)] for r in range(2)])
            imag = fold([[one[r][c][1] for c in range(2)] for r in range(2)])
            put_right(start, real, imag)
        right(0, 1)
        left(0, 0)
        for start in range(0, half, CHUNK):
            moved_real = fold(take(start, 0))
            moved_imag = fold(take(start, 1))
            real = [[None, None], [None, None]]
            imag = [[None, None], [None, None]]
            for r in range(2):
                for c in range(2):
                    mr, mi = moved_real[r][c], moved_imag[r][c]
                    moved_ref[0, at(r, start), lanes(c)] = mr
                    moved_ref[1, at(r, start), lanes(c)] = mi
                    tr, ti = window_ref[2, at(r, start), lanes(c)], window_ref[3, at(r, start), lanes(c)]
                    real[r][c] = mr * tr - mi * ti
                    imag[r][c] = mr * ti + mi * tr
            put_right(start, fold(real), fold(imag))
        right(1, 1)
        left(1, 0)
        for start in range(0, half, CHUNK):
            far_real, far_imag = take(start, 0), take(start, 1)
            real = [[None, None], [None, None]]
            imag = [[None, None], [None, None]]
            for p in range(2):
                for q in range(2):
                    fr, fi = far_real[p][q], far_imag[p][q]
                    misfit = fr * fr + fi * fi - measured_ref[slot, at(p, start), lanes(q)]
                    real[p][q] = misfit * fr
                    imag[p][q] = misfit * fi
            put_right(start, real, imag)
        right(1, 0)
        left(1, 1)

        def collect(start, k, quads):
            for r in range(2):
                edge = boundary(r, start)
                side = jnp.where(cols[0], jnp.where(cols[1], 0.0, quads[r][1]), quads[r][0])
                own = [jnp.where(cols[c], quads[r][c], 0.0) for c in range(2)]
                if edge:
                    mask = row_mask(r, start)
                    for c in range(2):
                        gcore_ref[k, at(r, start), lanes(c)] += jnp.where(mask, own[c], 0.0)
                        grow_ref[k, pl.ds(start, CHUNK), lanes(c)] += jnp.where(mask, 0.0, own[c])
                    gcol_ref[k, at(r, start), :] += jnp.where(mask, side, 0.0)
                    gcorner_ref[k, pl.ds(start, CHUNK), :] += jnp.where(mask, 0.0, side)
                else:
                    for c in range(2):
                        gcore_ref[k, at(r, start), lanes(c)] += own[c]
                    gcol_ref[k, at(r, start), :] += side

        def empty():
            return [[None, None], [None, None]]

        for start in range(0, half, CHUNK):
            back_real = fold(take(start, 0))
            back_imag = fold(take(start, 1))
            real, imag, two_real, two_imag = empty(), empty(), empty(), empty()
            for r in range(2):
                for c in range(2):
                    br, bi = back_real[r][c], back_imag[r][c]
                    mr, mi = moved_ref[0, at(r, start), lanes(c)], moved_ref[1, at(r, start), lanes(c)]
                    tr, ti = window_ref[2, at(r, start), lanes(c)], window_ref[3, at(r, start), lanes(c)]
                    two_real[r][c] = mr * br + mi * bi
                    two_imag[r][c] = mr * bi - mi * br
                    real[r][c] = tr * br + ti * bi
                    imag[r][c] = tr * bi - ti * br
            collect(start, 2, two_real)
            collect(start, 3, two_imag)
            put_right(start, fold(real), fold(imag))
        right(0, 0)
        left(0, 1)
        for start in range(0, half, CHUNK):
            wave_real = fold(take(start, 0))
            wave_imag = fold(take(start, 1))
            one_real, one_imag = empty(), empty()
            for r in range(2):
                for c in range(2):
                    wr, wi = wave_real[r][c], wave_imag[r][c]
                    pr, pi = rolled_ref[0, at(r, start), lanes(c)], rolled_ref[1, at(r, start), lanes(c)]
                    fr, fi = window_ref[0, at(r, start), lanes(c)], window_ref[1, at(r, start), lanes(c)]
                    one_real[r][c] = pr * wr + pi * wi
                    one_imag[r][c] = pr * wi - pi * wr
                    moved_ref[0, at(r, start), lanes(c)] = fr * wr + fi * wi
                    moved_ref[1, at(r, start), lanes(c)] = fr * wi - fi * wr
            collect(start, 0, one_real)
            collect(start, 1, one_imag)
        back_row = lax.rem(size - shift_row, size)
        back_col = lax.rem(size - shift_col, size)
        for comp in range(2):
            gprobe_ref[comp] += pltpu.roll(pltpu.roll(moved_ref[comp], back_row, 0), back_col, 1)
        return carry

    lax.fori_loop(0, count_ref[0], visit, 0)


def sort_measured(count, values, order):
    return pl.pallas_call(
        sort_kernel,
        out_shape=jax.ShapeDtypeStruct(values.shape, values.dtype),
        in_specs=[pl.BlockSpec(memory_space=pltpu.SMEM)] + [pl.BlockSpec(memory_space=pltpu.VMEM)] * 2,
        out_specs=pl.BlockSpec(memory_space=pltpu.VMEM),
        compiler_params=pltpu.CompilerParams(vmem_limit_bytes=32 * 1024 * 1024),
        name="sort_measured",
    )(count, values, order)


def gradients(count, offsets, core, row, col, corner, probe, measured, table):
    size = probe.shape[1]
    shapes = [x.shape for x in (core, row, col, corner, probe)]
    f32, bf16 = jnp.float32, jnp.bfloat16
    return pl.pallas_call(
        grad_kernel,
        out_shape=[jax.ShapeDtypeStruct(s, f32) for s in shapes],
        in_specs=[pl.BlockSpec(memory_space=pltpu.SMEM)] * 2 + [pl.BlockSpec(memory_space=pltpu.VMEM)] * 7,
        out_specs=[pl.BlockSpec(memory_space=pltpu.VMEM)] * 5,
        scratch_shapes=[
            pltpu.VMEM((4, size, size), f32),
            pltpu.VMEM((2, size, size), f32),
            pltpu.VMEM((2, size, size), f32),
            pltpu.VMEM((2, size, size), bf16),
            pltpu.VMEM((2, size, size), bf16),
            pltpu.VMEM((2, size, size), bf16),
            pltpu.VMEM((2, size, size), bf16),
            pltpu.VMEM((2, size, size), f32),
            pltpu.VMEM((2, size, size), f32),
        ],
        compiler_params=pltpu.CompilerParams(vmem_limit_bytes=48 * 1024 * 1024),
        name="gradients",
    )(count, offsets, core, row, col, corner, probe, measured, table)


def shifted(value, axis, step):
    count = lax.axis_size(axis)
    return lax.ppermute(value, axis, [(i, (i + step) % count) for i in range(count)])


def pack(value):
    rows = value.shape[1] // 2
    return jnp.concatenate([value[:, :rows], value[:, rows:]], axis=2)


def unpack(from_right, from_left):
    parts_of = [
        jnp.concatenate([from_right[..., s], from_left[..., s]], axis=2)
        for s in (slice(0, MARGIN), slice(MARGIN, None))
    ]
    return jnp.concatenate(parts_of, axis=1)


def swap_cols(to_left, to_right):
    return unpack(shifted(pack(to_left), "tx", -1), shifted(pack(to_right), "tx", 1))


def surroundings(core):
    size = core.shape[1]
    from_below = shifted(core[:, :MARGIN], "ty", -1)
    from_above = shifted(core[:, size - MARGIN :], "ty", 1)
    col = swap_cols(core[:, :, :MARGIN], core[:, :, size - MARGIN :])
    row = jnp.concatenate([from_below, from_above], axis=1)
    corner = swap_cols(row[:, :, :MARGIN], row[:, :, size - MARGIN :])
    return row, col, corner


def spread_cols(side, size):
    gap = jnp.zeros(side.shape[:2] + (size - 2 * MARGIN,), side.dtype)
    return jnp.concatenate([side[:, :, :MARGIN], gap, side[:, :, MARGIN:]], axis=2)


def gather_sums(gcore, grow, gcol, gcorner):
    size = gcore.shape[1]

    def to_owner(side):
        from_left = shifted(pack(side[:, :, :MARGIN]), "tx", 1)
        from_right = shifted(pack(side[:, :, MARGIN:]), "tx", -1)
        return spread_cols(unpack(from_left, from_right), size)

    grow = grow + to_owner(gcorner)
    from_above = shifted(grow[:, :MARGIN], "ty", 1)
    from_below = shifted(grow[:, MARGIN:], "ty", -1)
    total = gcore + to_owner(gcol)
    gap = jnp.zeros((gcore.shape[0], size - 2 * MARGIN, size), gcore.dtype)
    return total + jnp.concatenate([from_above, gap, from_below], axis=1)


def rounds(ty, tx):
    def split(axis, count, first):
        found, inner = [], 1
        while inner < count:
            members = first if inner == 1 and first else 4
            while (count // inner) % members:
                members //= 2
            if members < 2:
                members = count // inner
            found.append((axis, inner, members))
            inner *= members
        return found

    across = split("tx", tx, 2)
    return across[:1] + split("ty", ty, 0) + across[1:]


def ring(axis, inner, members, step):
    count = lax.axis_size(axis)
    pairs = []
    for i in range(count):
        low, mid, high = i % inner, (i // inner) % members, i // (inner * members)
        pairs.append((i, (high * members + (mid + step) % members) * inner + low))
    return pairs


def place(axis, inner, members):
    return (lax.axis_index(axis) // inner) % members


def scatter_round(value, axis, inner, members):
    pieces = value.reshape((members, value.shape[0] // members) + value.shape[1:])
    me = place(axis, inner, members)
    pick = lambda step: lax.dynamic_index_in_dim(pieces, (me + step) % members, 0, keepdims=False)
    out = pick(0)
    for got in [lax.ppermute(pick(s), axis, ring(axis, inner, members, s)) for s in range(1, members)]:
        out = out + got
    return out


def gather_round(value, axis, inner, members):
    me = place(axis, inner, members)
    got = [value] + [lax.ppermute(value, axis, ring(axis, inner, members, s)) for s in range(1, members)]
    out = jnp.zeros((members,) + value.shape, value.dtype)
    for step, piece in enumerate(got):
        out = lax.dynamic_update_index_in_dim(out, piece, (me + members - step) % members, 0)
    return out.reshape((members * value.shape[0],) + value.shape[1:])


def total_over_devices(value):
    flat = value.reshape(value.shape[0] * value.shape[1], value.shape[2])
    steps = rounds(lax.axis_size("ty"), lax.axis_size("tx"))
    for step in steps:
        flat = scatter_round(flat, *step)
    for step in reversed(steps):
        flat = gather_round(flat, *step)
    return flat.reshape(value.shape)


def make_body(table, order):
    def body(object_slices, probe, position_count, offsets, intensities):
        size = probe.shape[1]
        devices = lax.axis_size("ty") * lax.axis_size("tx")
        count = position_count.reshape(1)
        place_of = offsets.reshape(offsets.shape[2:])
        core = object_slices.reshape((4,) + object_slices.shape[2:])
        around = surroundings(core)
        measured = sort_measured(count, intensities.reshape(intensities.shape[2:]), order)
        for step in range(ITERS):
            *grads, gprobe = gradients(count, place_of, core, *around, probe, measured, table)
            peak = jnp.max(probe[0] * probe[0] + probe[1] * probe[1]) + 1e-06
            core = core - object_rate / peak * gather_sums(*grads)
            if step + 1 < ITERS:
                around = surroundings(core)
            probe = probe - probe_rate / devices * total_over_devices(gprobe)
        return core.reshape(object_slices.shape), probe

    return body


def solution(mesh):
    size = 256
    table, order = tables(size), lane_order(size)

    def run(object_slices, probe, position_count, offsets, intensities):
        placed = (
            P(None, None, "ty", "tx"),
            P(),
            P("ty", "tx"),
            P("ty", "tx", None, None),
            P("ty", "tx", None, None, None),
        )
        return jax.shard_map(
            make_body(jnp.asarray(table), jnp.asarray(order)),
            mesh=mesh,
            in_specs=placed,
            out_specs=(P(None, None, "ty", "tx"), P()),
            check_vma=False,
        )(object_slices, probe, position_count, offsets, intensities)

    return run
```

```python
import math

import jax
import jax.numpy as jnp
import ml_dtypes
import numpy as np
from jax import lax
from jax.experimental import pallas as pl
from jax.experimental.pallas import tpu as pltpu
from jax.sharding import PartitionSpec as P

MARGIN = 64
ITERS = 2
CHUNK = 16

chirp_rate = 0.5
object_rate = 0.5
probe_rate = 2.0


def tables(size):
    index = np.arange(size)
    four = np.exp(-2j * np.pi * (np.outer(index, index) % size) / size) / math.sqrt(size)
    centred = (index + size // 2) % size - size // 2
    kernel = np.exp(-1j * chirp_rate * np.pi * centred * centred / size)
    prop = (four.conj() * kernel[None, :]) @ four
    half = size // 2
    near, far = prop[:half, :half], prop[:half, half:]
    blocks = ((0.5 * (near + far), 0.5 * (near - far)), (four[0::2, :half], four[1::2, :half]))
    out = np.zeros((2, 2, 2, 2, size, size), ml_dtypes.bfloat16)
    for family in range(2):
        for parity in range(2):
            block = blocks[family][parity]
            left = np.block([[block.real, -block.imag], [block.imag, block.real]])
            for form, value in enumerate((left, left.T)):
                high = value.astype(np.float32).astype(ml_dtypes.bfloat16)
                low = (value - high.astype(np.float64)).astype(np.float32).astype(ml_dtypes.bfloat16)
                out[family, parity, form, 0] = high
                out[family, parity, form, 1] = low
    return out


def lane_order(size):
    out = np.zeros((size, size), ml_dtypes.bfloat16)
    half = size // 2
    for lane in range(half):
        out[2 * lane, lane] = 1
        out[2 * lane + 1, half + lane] = 1
    return np.stack([out, out.T])


def dot(left, right):
    return jnp.dot(left, right, preferred_element_type=jnp.float32)


def parts(value):
    high = value.astype(jnp.bfloat16)
    low = (value - high.astype(jnp.float32)).astype(jnp.bfloat16)
    return high, low


def thirds(value):
    first = value.astype(jnp.bfloat16)
    rest = value - first.astype(jnp.float32)
    second = rest.astype(jnp.bfloat16)
    return first, second, (rest - second.astype(jnp.float32)).astype(jnp.bfloat16)


def sort_kernel(count_ref, values_ref, order_ref, out_ref):
    out_ref[...] = jnp.zeros_like(out_ref)

    def visit(slot, carry):
        first, second, third = [dot(x, order_ref[0]) for x in thirds(values_ref[slot])]
        first, second, third = [dot(order_ref[1], x) for x in thirds((first + second) + third)]
        out_ref[slot] = (first + second) + third
        return carry

    lax.fori_loop(0, count_ref[0], visit, 0)


def common(size):
    half, quarter = size // 2, size // 4

    def at(part, start):
        return pl.ds(part * half + start, CHUNK)

    def lanes(part):
        return pl.ds(part * half, half)

    def boundary(part, start):
        return (start < quarter) == (part == 0)

    return half, at, lanes, boundary


def fold(quads):
    mixed = [[quads[0][c] + quads[1][c] for c in range(2)], [quads[0][c] - quads[1][c] for c in range(2)]]
    return [[m[0] + m[1], m[0] - m[1]] for m in mixed]


def empty():
    return [[None, None], [None, None]]


def masks(size, top, lead):
    half = size // 2
    lane = lax.broadcasted_iota(jnp.int32, (CHUNK, half), 1)
    row = lax.broadcasted_iota(jnp.int32, (CHUNK, half), 0)
    cols = (lane + MARGIN >= lead, lane - MARGIN < lead)

    def row_mask(part, start):
        inside = row + start
        return inside + MARGIN >= top if part == 0 else inside - MARGIN < top

    return cols, row_mask


def stages(size, table_ref, high_ref, low_ref, rhigh_ref, rlow_ref, mid_ref, back_ref):
    half, at, lanes, _ = common(size)

    def put(start, real, imag):
        for p in range(2):
            for q in range(2):
                for comp, value in ((0, real[p][q]), (1, imag[p][q])):
                    high, low = parts(value)
                    high_ref[q, at(p, start), lanes(comp)] = high
                    low_ref[q, at(p, start), lanes(comp)] = low

    def run(family, form):
        for q in range(2):
            weight, small = table_ref[family, q, form, 0], table_ref[family, q, form, 1]
            mid_ref[q] = dot(high_ref[q], weight) + dot(low_ref[q], weight) + dot(high_ref[q], small)
        for q in range(2):
            for p in range(2):
                for start in range(0, half, CHUNK):
                    for comp in range(2):
                        high, low = parts(mid_ref[q, at(p, start), lanes(comp)])
                        rhigh_ref[p, at(comp, start), lanes(q)] = high
                        rlow_ref[p, at(comp, start), lanes(q)] = low
        for p in range(2):
            weight, small = table_ref[family, p, 1 - form, 0], table_ref[family, p, 1 - form, 1]
            back_ref[p] = dot(weight, rhigh_ref[p]) + dot(small, rhigh_ref[p]) + dot(weight, rlow_ref[p])

    def take(start, comp):
        return [[back_ref[p, at(comp, start), lanes(q)] for q in range(2)] for p in range(2)]

    return put, run, take


def window_of(size, core_ref, row_ref, col_ref, corner_ref, cols, row_mask):
    half, at, lanes, boundary = common(size)

    def window(start, k):
        out = empty()
        for r in range(2):
            other = col_ref[k, at(r, start), :]
            if boundary(r, start):
                mask = row_mask(r, start)
                other = jnp.where(mask, other, corner_ref[k, pl.ds(start, CHUNK), :])
            for c in range(2):
                own = core_ref[k, at(r, start), lanes(c)]
                if boundary(r, start):
                    own = jnp.where(mask, own, row_ref[k, pl.ds(start, CHUNK), lanes(c)])
                out[r][c] = jnp.where(cols[c], own, other)
        return out

    return window


def collect_into(size, gcore_ref, grow_ref, gcol_ref, gcorner_ref, cols, row_mask):
    half, at, lanes, boundary = common(size)

    def collect(start, k, quads):
        for r in range(2):
            side = jnp.where(cols[0], jnp.where(cols[1], 0.0, quads[r][1]), quads[r][0])
            own = [jnp.where(cols[c], quads[r][c], 0.0) for c in range(2)]
            if boundary(r, start):
                mask = row_mask(r, start)
                for c in range(2):
                    gcore_ref[k, at(r, start), lanes(c)] += jnp.where(mask, own[c], 0.0)
                    grow_ref[k, pl.ds(start, CHUNK), lanes(c)] += jnp.where(mask, 0.0, own[c])
                gcol_ref[k, at(r, start), :] += jnp.where(mask, side, 0.0)
                gcorner_ref[k, pl.ds(start, CHUNK), :] += jnp.where(mask, 0.0, side)
            else:
                for c in range(2):
                    gcore_ref[k, at(r, start), lanes(c)] += own[c]
                gcol_ref[k, at(r, start), :] += side

    return collect


TILE = 8


def roller(size, shift_row, shift_col, twice_ref):
    half = size // 2
    lane = lax.broadcasted_iota(jnp.int32, (TILE, half), 1)
    far = (shift_col >= half).astype(jnp.int32)
    step = shift_col - far * half
    other = (lane < step).astype(jnp.int32) != far
    whole = shift_row // TILE
    rest = shift_row - whole * TILE
    row = lax.broadcasted_iota(jnp.int32, (CHUNK, size), 0)
    early = lax.rem(row, TILE) < rest

    def put(k, start, low, high):
        low, high = pltpu.roll(low, step, 1), pltpu.roll(high, step, 1)
        turned = (jnp.where(other, high, low), jnp.where(other, low, high))
        for c in range(2):
            value = pltpu.roll(turned[c], rest, 0)
            twice_ref[k, start : start + TILE, c * half : (c + 1) * half] = value
            twice_ref[k, size + start : size + start + TILE, c * half : (c + 1) * half] = value

    def take(k, start):
        first = pl.multiple_of((size // TILE + start // TILE - 1 - whole) * TILE, TILE)
        rows = twice_ref[k, pl.ds(first, CHUNK + TILE), :]
        return jnp.where(early, rows[:CHUNK], rows[TILE:])

    return put, take


def shifts(size, top, lead):
    return lax.rem(top + (size - MARGIN), size), lax.rem(lead + (size - MARGIN), size)


def grad_kernel(
    count_ref, offset_ref, core_ref, row_ref, col_ref, corner_ref, probe_ref, measured_ref, table_ref,
    gcore_ref, grow_ref, gcol_ref, gcorner_ref, gprobe_ref,
    window_ref, moved_ref, rolled_ref, twice_ref, *work,
):
    size = probe_ref.shape[1]
    half, at, lanes, _ = common(size)
    put, run, take = stages(size, table_ref, *work)
    for ref in (gcore_ref, grow_ref, gcol_ref, gcorner_ref, gprobe_ref):
        ref[...] = jnp.zeros_like(ref)

    def visit(slot, carry):
        top, lead = offset_ref[slot, 0], offset_ref[slot, 1]
        shift_row, shift_col = shifts(size, top, lead)
        cols, row_mask = masks(size, top, lead)
        window = window_of(size, core_ref, row_ref, col_ref, corner_ref, cols, row_mask)
        collect = collect_into(size, gcore_ref, grow_ref, gcol_ref, gcorner_ref, cols, row_mask)
        roll_put, roll_take = roller(size, shift_row, shift_col, twice_ref)
        for k in range(2):
            for start in range(0, size, TILE):
                roll_put(k, start, *[probe_ref[k, pl.ds(start, TILE), lanes(c)] for c in range(2)])
        for start in range(0, half, CHUNK):
            one_real, one_imag = window(start, 0), window(start, 1)
            real, imag = empty(), empty()
            for r in range(2):
                turned = [roll_take(k, r * half + start) for k in range(2)]
                for c in range(2):
                    pr, pi = [t[:, c * half : (c + 1) * half] for t in turned]
                    wr, wi = one_real[r][c], one_imag[r][c]
                    rolled_ref[0, at(r, start), lanes(c)] = pr
                    rolled_ref[1, at(r, start), lanes(c)] = pi
                    window_ref[0, at(r, start), lanes(c)] = wr
                    window_ref[1, at(r, start), lanes(c)] = wi
                    real[r][c] = pr * wr - pi * wi
                    imag[r][c] = pr * wi + pi * wr
            put(start, fold(real), fold(imag))
        run(0, 1)
        for start in range(0, half, CHUNK):
            moved_real, moved_imag = fold(take(start, 0)), fold(take(start, 1))
            two_real, two_imag = window(start, 2), window(start, 3)
            real, imag = empty(), empty()
            for r in range(2):
                for c in range(2):
                    mr, mi = moved_real[r][c], moved_imag[r][c]
                    tr, ti = two_real[r][c], two_imag[r][c]
                    moved_ref[0, at(r, start), lanes(c)] = mr
                    moved_ref[1, at(r, start), lanes(c)] = mi
                    window_ref[2, at(r, start), lanes(c)] = tr
                    window_ref[3, at(r, start), lanes(c)] = ti
                    real[r][c] = mr * tr - mi * ti
                    imag[r][c] = mr * ti + mi * tr
            put(start, fold(real), fold(imag))
        run(1, 1)
        for start in range(0, half, CHUNK):
            far_real, far_imag = take(start, 0), take(start, 1)
            real, imag = empty(), empty()
            for p in range(2):
                for q in range(2):
                    fr, fi = far_real[p][q], far_imag[p][q]
                    misfit = fr * fr + fi * fi - measured_ref[slot, at(p, start), lanes(q)]
                    real[p][q] = misfit * fr
                    imag[p][q] = misfit * fi
            put(start, real, imag)
        run(1, 0)
        for start in range(0, half, CHUNK):
            back_real, back_imag = fold(take(start, 0)), fold(take(start, 1))
            real, imag, two_real, two_imag = empty(), empty(), empty(), empty()
            for r in range(2):
                for c in range(2):
                    br, bi = back_real[r][c], back_imag[r][c]
                    mr, mi = [moved_ref[k, at(r, start), lanes(c)] for k in range(2)]
                    tr, ti = [window_ref[k, at(r, start), lanes(c)] for k in (2, 3)]
                    two_real[r][c] = mr * br + mi * bi
                    two_imag[r][c] = mr * bi - mi * br
                    real[r][c] = tr * br + ti * bi
                    imag[r][c] = tr * bi - ti * br
            put(start, fold(real), fold(imag))
            collect(start, 2, two_real)
            collect(start, 3, two_imag)
        run(0, 0)
        roll_put, roll_take = roller(
            size, lax.rem(size - shift_row, size), lax.rem(size - shift_col, size), twice_ref
        )
        for start in range(0, half, CHUNK):
            wave_real, wave_imag = fold(take(start, 0)), fold(take(start, 1))
            one_real, one_imag = empty(), empty()
            for r in range(2):
                turned = empty()
                for c in range(2):
                    wr, wi = wave_real[r][c], wave_imag[r][c]
                    pr, pi = [rolled_ref[k, at(r, start), lanes(c)] for k in range(2)]
                    fr, fi = [window_ref[k, at(r, start), lanes(c)] for k in range(2)]
                    one_real[r][c] = pr * wr + pi * wi
                    one_imag[r][c] = pr * wi - pi * wr
                    turned[0][c] = fr * wr + fi * wi
                    turned[1][c] = fr * wi - fi * wr
                for k in range(2):
                    for tile in range(0, CHUNK, TILE):
                        roll_put(k, r * half + start + tile, *[t[tile : tile + TILE] for t in turned[k]])
            collect(start, 0, one_real)
            collect(start, 1, one_imag)
        for k in range(2):
            for start in range(0, size, CHUNK):
                gprobe_ref[k, start : start + CHUNK, :] += roll_take(k, start)
        return carry

    lax.fori_loop(0, count_ref[0], visit, 0)


def sort_measured(count, values, order):
    return pl.pallas_call(
        sort_kernel,
        out_shape=jax.ShapeDtypeStruct(values.shape, values.dtype),
        in_specs=[pl.BlockSpec(memory_space=pltpu.SMEM)] + [pl.BlockSpec(memory_space=pltpu.VMEM)] * 2,
        out_specs=pl.BlockSpec(memory_space=pltpu.VMEM),
        compiler_params=pltpu.CompilerParams(vmem_limit_bytes=16 * 1024 * 1024),
        name="sort_measured",
    )(count, values, order)


def call(kernel, name, inputs, scalars, outputs, scratch, size, products):
    f32, bf16 = jnp.float32, jnp.bfloat16
    vmem = pl.BlockSpec(memory_space=pltpu.VMEM)
    work = [pltpu.VMEM((2, size, size), bf16)] * 4 + [pltpu.VMEM((2, size, size), f32)] * 2
    return pl.pallas_call(
        kernel,
        out_shape=[jax.ShapeDtypeStruct(s, f32) for s in outputs],
        in_specs=[pl.BlockSpec(memory_space=pltpu.SMEM)] * scalars + [vmem] * (len(inputs) - scalars),
        out_specs=[vmem] * len(outputs),
        scratch_shapes=[pltpu.VMEM(s, f32) for s in scratch] + work,
        compiler_params=pltpu.CompilerParams(vmem_limit_bytes=16 * 1024 * 1024),
        cost_estimate=pl.CostEstimate(
            flops=products * 2 * size**3, transcendentals=0, bytes_accessed=sum(x.size * 4 for x in inputs)
        ),
        name=name,
    )(*inputs)


def shifted(value, axis, step):
    count = lax.axis_size(axis)
    return lax.ppermute(value, axis, [(i, (i + step) % count) for i in range(count)])


def pack(value):
    rows = value.shape[1] // 2
    return jnp.concatenate([value[:, :rows], value[:, rows:]], axis=2)


def unpack(from_right, from_left):
    parts_of = [
        jnp.concatenate([from_right[..., s], from_left[..., s]], axis=2)
        for s in (slice(0, MARGIN), slice(MARGIN, None))
    ]
    return jnp.concatenate(parts_of, axis=1)


def swap_cols(to_left, to_right):
    return unpack(shifted(pack(to_left), "tx", -1), shifted(pack(to_right), "tx", 1))


def sides(core):
    size = core.shape[1]
    from_below = shifted(core[:, :MARGIN], "ty", -1)
    from_above = shifted(core[:, size - MARGIN :], "ty", 1)
    col = swap_cols(core[:, :, :MARGIN], core[:, :, size - MARGIN :])
    return jnp.concatenate([from_below, from_above], axis=1), col


def corners(row):
    return swap_cols(row[:, :, :MARGIN], row[:, :, row.shape[2] - MARGIN :])


def owned_cols(side):
    from_left = shifted(pack(side[:, :, :MARGIN]), "tx", 1)
    from_right = shifted(pack(side[:, :, MARGIN:]), "tx", -1)
    return unpack(from_left, from_right)


def owned_rows(side):
    return shifted(side[:, :MARGIN], "ty", 1), shifted(side[:, MARGIN:], "ty", -1)


def spread_cols(side, size):
    gap = jnp.zeros(side.shape[:2] + (size - 2 * MARGIN,), side.dtype)
    return jnp.concatenate([side[:, :, :MARGIN], gap, side[:, :, MARGIN:]], axis=2)


def spread_rows(low, high, size):
    gap = jnp.zeros((low.shape[0], size - 2 * MARGIN, low.shape[2]), low.dtype)
    return jnp.concatenate([low, gap, high], axis=1)


def split(count, inner):
    found = []
    while inner < count:
        members = 4 if (count // inner) % 4 == 0 else 2
        found.append((inner, members))
        inner *= members
    return found


def ring(axis, inner, members, step):
    count = lax.axis_size(axis)
    pairs = []
    for i in range(count):
        low, mid, high = i % inner, (i // inner) % members, i // (inner * members)
        pairs.append((i, (high * members + (mid + step) % members) * inner + low))
    return pairs


def place(axis, inner, members):
    return (lax.axis_index(axis) // inner) % members


def scatter_round(value, axis, inner, members):
    pieces = value.reshape((members, value.shape[0] // members) + value.shape[1:])
    me = place(axis, inner, members)
    pick = lambda step: lax.dynamic_index_in_dim(pieces, (me + step) % members, 0, keepdims=False)
    out = pick(0)
    for got in [lax.ppermute(pick(s), axis, ring(axis, inner, members, s)) for s in range(1, members)]:
        out = out + got
    return out


def gather_round(value, axis, inner, members):
    me = place(axis, inner, members)
    got = [value] + [lax.ppermute(value, axis, ring(axis, inner, members, s)) for s in range(1, members)]
    out = jnp.zeros((members,) + value.shape, value.dtype)
    for step, piece in enumerate(got):
        out = lax.dynamic_update_index_in_dim(out, piece, (me + members - step) % members, 0)
    return out.reshape((members * value.shape[0],) + value.shape[1:])


def doubling_round(value, axis, distance):
    count = lax.axis_size(axis)
    return value + lax.ppermute(value, axis, [(i, i ^ distance) for i in range(count)])


def total_over_devices(value, held):
    flat = value.reshape(value.shape[0] * value.shape[1], value.shape[2])
    ty, tx = lax.axis_size("ty"), lax.axis_size("tx")
    steps = [("tx", 1, 2)] + [("tx", *s) for s in split(tx, 2)]
    for step in steps:
        flat = scatter_round(flat, *step)
    distance = 1
    while distance < ty:
        flat = doubling_round(flat, "ty", distance)
        if distance == 1:
            flat, held = lax.optimization_barrier((flat, held))
        distance *= 2
    for step in reversed(steps):
        flat = gather_round(flat, *step)
    return flat.reshape(value.shape), held


def make_body(table, order):
    def body(object_slices, probe, position_count, offsets, intensities):
        size = probe.shape[1]
        devices = lax.axis_size("ty") * lax.axis_size("tx")
        count = position_count.reshape(1)
        place_of = offsets.reshape(offsets.shape[2:])
        core = object_slices.reshape((4,) + object_slices.shape[2:])
        measured = sort_measured(count, intensities.reshape(intensities.shape[2:]), order)
        row, col = sides(core)
        for step in range(ITERS):
            inputs = (count, place_of, core, row, col, corners(row), probe, measured, table)
            plane, field = (2, size, size), (4, size, size)
            gcore, grow, gcol, gcorner, gprobe = call(
                grad_kernel, "gradients", inputs, 2, [x.shape for x in inputs[2:7]],
                [field, plane, plane, (2, 2 * size, size)], size, 240,
            )
            peak = jnp.max(probe[0] * probe[0] + probe[1] * probe[1]) + 1e-06
            low, high = owned_rows(grow + spread_cols(owned_cols(gcorner), size))
            total = gcore + spread_cols(owned_cols(gcol), size) + spread_rows(low, high, size)
            core = core - object_rate / peak * total
            summed, core = total_over_devices(gprobe, core)
            if step + 1 < ITERS:
                row, col = sides(core)
            probe = probe - probe_rate / devices * summed
        return core.reshape(object_slices.shape), probe

    return body


def solution(mesh):
    size = 256
    table, order = tables(size), lane_order(size)

    def run(object_slices, probe, position_count, offsets, intensities):
        placed = (
            P(None, None, "ty", "tx"),
            P(),
            P("ty", "tx"),
            P("ty", "tx", None, None),
            P("ty", "tx", None, None, None),
        )
        return jax.shard_map(
            make_body(jnp.asarray(table), jnp.asarray(order)),
            mesh=mesh,
            in_specs=placed,
            out_specs=(P(None, None, "ty", "tx"), P()),
            check_vma=False,
        )(object_slices, probe, position_count, offsets, intensities)

    return run
```

```python
import math

import jax
import jax.numpy as jnp
import ml_dtypes
import numpy as np
from jax import lax
from jax.experimental import pallas as pl
from jax.experimental.pallas import tpu as pltpu
from jax.sharding import PartitionSpec as P

MARGIN = 64
ITERS = 2
CHUNK = 16
SKEW = 0

chirp_rate = 0.5
object_rate = 0.5
probe_rate = 2.0


def tables(size):
    index = np.arange(size)
    four = np.exp(-2j * np.pi * (np.outer(index, index) % size) / size) / math.sqrt(size)
    centred = (index + size // 2) % size - size // 2
    kernel = np.exp(-1j * chirp_rate * np.pi * centred * centred / size)
    prop = (four.conj() * kernel[None, :]) @ four
    half = size // 2
    near, far = prop[:half, :half], prop[:half, half:]
    blocks = ((0.5 * (near + far), 0.5 * (near - far)), (four[0::2, :half], four[1::2, :half]))
    out = np.zeros((2, 2, 2, 2, size, size), ml_dtypes.bfloat16)
    for family in range(2):
        for parity in range(2):
            block = blocks[family][parity]
            left = np.block([[block.real, -block.imag], [block.imag, block.real]])
            for form, value in enumerate((left, left.T)):
                high = value.astype(np.float32).astype(ml_dtypes.bfloat16)
                low = (value - high.astype(np.float64)).astype(np.float32).astype(ml_dtypes.bfloat16)
                out[family, parity, form, 0] = high
                out[family, parity, form, 1] = low
    return out


def lane_order(size):
    out = np.zeros((size, size), ml_dtypes.bfloat16)
    half = size // 2
    for lane in range(half):
        out[2 * lane, lane] = 1
        out[2 * lane + 1, half + lane] = 1
    return np.stack([out, out.T])


def dot(left, right):
    return jnp.dot(left, right, preferred_element_type=jnp.float32)


def parts(value):
    high = value.astype(jnp.bfloat16)
    low = (value - high.astype(jnp.float32)).astype(jnp.bfloat16)
    return high, low


def thirds(value):
    first = value.astype(jnp.bfloat16)
    rest = value - first.astype(jnp.float32)
    second = rest.astype(jnp.bfloat16)
    return first, second, (rest - second.astype(jnp.float32)).astype(jnp.bfloat16)


def sort_kernel(count_ref, values_ref, order_ref, out_ref):
    out_ref[...] = jnp.zeros_like(out_ref)

    def visit(slot, carry):
        first, second, third = [dot(x, order_ref[0]) for x in thirds(values_ref[slot])]
        first, second, third = [dot(order_ref[1], x) for x in thirds((first + second) + third)]
        out_ref[slot] = (first + second) + third
        return carry

    lax.fori_loop(0, count_ref[0], visit, 0)


def common(size):
    half, quarter = size // 2, size // 4

    def at(part, start):
        return pl.ds(part * half + start, CHUNK)

    def lanes(part):
        return pl.ds(part * half, half)

    def boundary(part, start):
        return (start < quarter) == (part == 0)

    return half, at, lanes, boundary


def fold(quads):
    mixed = [[quads[0][c] + quads[1][c] for c in range(2)], [quads[0][c] - quads[1][c] for c in range(2)]]
    return [[m[0] + m[1], m[0] - m[1]] for m in mixed]


def empty():
    return [[None, None], [None, None]]


def masks(size, top, lead):
    half = size // 2
    lane = lax.broadcasted_iota(jnp.int32, (CHUNK, half), 1)
    row = lax.broadcasted_iota(jnp.int32, (CHUNK, half), 0)
    cols = (lane + MARGIN >= lead, lane - MARGIN < lead)

    def row_mask(part, start):
        inside = row + start
        return inside + MARGIN >= top if part == 0 else inside - MARGIN < top

    return cols, row_mask


def stages(size, table_ref, high_ref, low_ref, rhigh_ref, rlow_ref, mid_ref, back_ref):
    half, at, lanes, _ = common(size)

    def put(start, real, imag):
        for p in range(2):
            for q in range(2):
                for comp, value in ((0, real[p][q]), (1, imag[p][q])):
                    high, low = parts(value)
                    high_ref[q, at(p, start), lanes(comp)] = high
                    low_ref[q, at(p, start), lanes(comp)] = low

    def right(family, form):
        for q in range(2):
            weight, small = table_ref[family, q, form, 0], table_ref[family, q, form, 1]
            mid_ref[q] = dot(high_ref[q], weight) + dot(low_ref[q], weight) + dot(high_ref[q], small)
        for q in range(2):
            for p in range(2):
                for start in range(0, half, CHUNK):
                    for comp in range(2):
                        high, low = parts(mid_ref[q, at(p, start), lanes(comp)])
                        rhigh_ref[p, at(comp, start), lanes(q)] = high
                        rlow_ref[p, at(comp, start), lanes(q)] = low

    def left(family, form):
        for p in range(2):
            weight, small = table_ref[family, p, 1 - form, 0], table_ref[family, p, 1 - form, 1]
            back_ref[p] = dot(weight, rhigh_ref[p]) + dot(small, rhigh_ref[p]) + dot(weight, rlow_ref[p])

    def take(start, comp):
        return [[back_ref[p, at(comp, start), lanes(q)] for q in range(2)] for p in range(2)]

    return put, right, left, take


def window_of(size, core_ref, row_ref, col_ref, corner_ref, cols, row_mask):
    half, at, lanes, boundary = common(size)

    def window(start, k):
        out = empty()
        for r in range(2):
            other = col_ref[k, at(r, start), :]
            if boundary(r, start):
                mask = row_mask(r, start)
                other = jnp.where(mask, other, corner_ref[k, pl.ds(start, CHUNK), :])
            for c in range(2):
                own = core_ref[k, at(r, start), lanes(c)]
                if boundary(r, start):
                    own = jnp.where(mask, own, row_ref[k, pl.ds(start, CHUNK), lanes(c)])
                out[r][c] = jnp.where(cols[c], own, other)
        return out

    return window


def collect_into(size, gcore_ref, grow_ref, gcol_ref, gcorner_ref, cols, row_mask):
    half, at, lanes, boundary = common(size)

    def collect(start, k, quads):
        for r in range(2):
            side = jnp.where(cols[0], jnp.where(cols[1], 0.0, quads[r][1]), quads[r][0])
            own = [jnp.where(cols[c], quads[r][c], 0.0) for c in range(2)]
            if boundary(r, start):
                mask = row_mask(r, start)
                for c in range(2):
                    gcore_ref[k, at(r, start), lanes(c)] += jnp.where(mask, own[c], 0.0)
                    grow_ref[k, pl.ds(start, CHUNK), lanes(c)] += jnp.where(mask, 0.0, own[c])
                gcol_ref[k, at(r, start), :] += jnp.where(mask, side, 0.0)
                gcorner_ref[k, pl.ds(start, CHUNK), :] += jnp.where(mask, 0.0, side)
            else:
                for c in range(2):
                    gcore_ref[k, at(r, start), lanes(c)] += own[c]
                gcol_ref[k, at(r, start), :] += side

    return collect


TILE = 8


def roller(size, shift_row, shift_col, twice_ref):
    half = size // 2
    lane = lax.broadcasted_iota(jnp.int32, (TILE, half), 1)
    far = (shift_col >= half).astype(jnp.int32)
    step = shift_col - far * half
    other = (lane < step).astype(jnp.int32) != far
    whole = shift_row // TILE
    rest = shift_row - whole * TILE
    row = lax.broadcasted_iota(jnp.int32, (CHUNK, size), 0)
    early = lax.rem(row, TILE) < rest

    def put(k, start, low, high):
        low, high = pltpu.roll(low, step, 1), pltpu.roll(high, step, 1)
        turned = (jnp.where(other, high, low), jnp.where(other, low, high))
        for c in range(2):
            value = pltpu.roll(turned[c], rest, 0)
            twice_ref[k, start : start + TILE, c * half : (c + 1) * half] = value

    def take(k, start):
        tiles = [
            pl.multiple_of(lax.rem(size + start + step * TILE - whole * TILE, size), TILE)
            for step in range(-1, CHUNK // TILE)
        ]
        rows = jnp.concatenate([twice_ref[k, pl.ds(tile, TILE), :] for tile in tiles], axis=0)
        return jnp.where(early, rows[:CHUNK], rows[TILE:])

    return put, take


def shifts(size, top, lead):
    return lax.rem(top + (size - MARGIN), size), lax.rem(lead + (size - MARGIN), size)


def grad_kernel(
    count_ref, offset_ref, core_ref, row_ref, col_ref, corner_ref, probe_ref, measured_ref, table_ref,
    gcore_ref, grow_ref, gcol_ref, gcorner_ref, gprobe_ref, *scratch,
):
    size = probe_ref.shape[1]
    half, at, lanes, _ = common(size)
    sets = [scratch[: len(scratch) // 2], scratch[len(scratch) // 2 :]]
    for ref in (gcore_ref, grow_ref, gcol_ref, gcorner_ref, gprobe_ref):
        ref[...] = jnp.zeros_like(ref)

    def position(slot, valid, window_ref, moved_ref, rolled_ref, twice_ref, *work):
        put, right, left, take = stages(size, table_ref, *work)
        found = []
        stage = found.append
        top, lead = offset_ref[slot, 0], offset_ref[slot, 1]
        shift_row, shift_col = shifts(size, top, lead)
        cols, row_mask = masks(size, top, lead)
        window = window_of(size, core_ref, row_ref, col_ref, corner_ref, cols, row_mask)
        collect = collect_into(size, gcore_ref, grow_ref, gcol_ref, gcorner_ref, cols, row_mask)
        roll_put, roll_take = roller(size, shift_row, shift_col, twice_ref)

        def part_1():
            for k in range(2):
                for start in range(0, size, TILE):
                    roll_put(k, start, *[probe_ref[k, pl.ds(start, TILE), lanes(c)] for c in range(2)])
            for start in range(0, half, CHUNK):
                one_real, one_imag = window(start, 0), window(start, 1)
                real, imag = empty(), empty()
                for r in range(2):
                    turned = [roll_take(k, r * half + start) for k in range(2)]
                    for c in range(2):
                        pr, pi = [t[:, c * half : (c + 1) * half] for t in turned]
                        wr, wi = one_real[r][c], one_imag[r][c]
                        rolled_ref[0, at(r, start), lanes(c)] = pr
                        rolled_ref[1, at(r, start), lanes(c)] = pi
                        window_ref[0, at(r, start), lanes(c)] = wr
                        window_ref[1, at(r, start), lanes(c)] = wi
                        real[r][c] = pr * wr - pi * wi
                        imag[r][c] = pr * wi + pi * wr
                put(start, fold(real), fold(imag))
        stage(part_1)

        stage(lambda: right(0, 1))
        stage(lambda: left(0, 1))
        def part_2():
            for start in range(0, half, CHUNK):
                moved_real, moved_imag = fold(take(start, 0)), fold(take(start, 1))
                two_real, two_imag = window(start, 2), window(start, 3)
                real, imag = empty(), empty()
                for r in range(2):
                    for c in range(2):
                        mr, mi = moved_real[r][c], moved_imag[r][c]
                        tr, ti = two_real[r][c], two_imag[r][c]
                        moved_ref[0, at(r, start), lanes(c)] = mr
                        moved_ref[1, at(r, start), lanes(c)] = mi
                        window_ref[2, at(r, start), lanes(c)] = tr
                        window_ref[3, at(r, start), lanes(c)] = ti
                        real[r][c] = mr * tr - mi * ti
                        imag[r][c] = mr * ti + mi * tr
                put(start, fold(real), fold(imag))
        stage(part_2)

        stage(lambda: right(1, 1))
        stage(lambda: left(1, 1))
        def part_3():
            for start in range(0, half, CHUNK):
                far_real, far_imag = take(start, 0), take(start, 1)
                real, imag = empty(), empty()
                for p in range(2):
                    for q in range(2):
                        fr, fi = far_real[p][q], far_imag[p][q]
                        misfit = fr * fr + fi * fi - measured_ref[slot, at(p, start), lanes(q)]
                        if valid is not None:
                            misfit = jnp.where(valid, misfit, 0.0)
                        real[p][q] = misfit * fr
                        imag[p][q] = misfit * fi
                put(start, real, imag)
        stage(part_3)

        stage(lambda: right(1, 0))
        stage(lambda: left(1, 0))
        def part_4():
            for start in range(0, half, CHUNK):
                back_real, back_imag = fold(take(start, 0)), fold(take(start, 1))
                real, imag, two_real, two_imag = empty(), empty(), empty(), empty()
                for r in range(2):
                    for c in range(2):
                        br, bi = back_real[r][c], back_imag[r][c]
                        mr, mi = [moved_ref[k, at(r, start), lanes(c)] for k in range(2)]
                        tr, ti = [window_ref[k, at(r, start), lanes(c)] for k in (2, 3)]
                        two_real[r][c] = mr * br + mi * bi
                        two_imag[r][c] = mr * bi - mi * br
                        real[r][c] = tr * br + ti * bi
                        imag[r][c] = tr * bi - ti * br
                put(start, fold(real), fold(imag))
                collect(start, 2, two_real)
                collect(start, 3, two_imag)
        stage(part_4)

        stage(lambda: right(0, 0))
        stage(lambda: left(0, 0))
        def part_5():
            roll_put, roll_take = roller(
                size, lax.rem(size - shift_row, size), lax.rem(size - shift_col, size), twice_ref
            )
            for start in range(0, half, CHUNK):
                wave_real, wave_imag = fold(take(start, 0)), fold(take(start, 1))
                one_real, one_imag = empty(), empty()
                for r in range(2):
                    turned = empty()
                    for c in range(2):
                        wr, wi = wave_real[r][c], wave_imag[r][c]
                        pr, pi = [rolled_ref[k, at(r, start), lanes(c)] for k in range(2)]
                        fr, fi = [window_ref[k, at(r, start), lanes(c)] for k in range(2)]
                        one_real[r][c] = pr * wr + pi * wi
                        one_imag[r][c] = pr * wi - pi * wr
                        turned[0][c] = fr * wr + fi * wi
                        turned[1][c] = fr * wi - fi * wr
                    for k in range(2):
                        for tile in range(0, CHUNK, TILE):
                            roll_put(k, r * half + start + tile, *[t[tile : tile + TILE] for t in turned[k]])
                collect(start, 0, one_real)
                collect(start, 1, one_imag)
            for k in range(2):
                for start in range(0, size, CHUNK):
                    gprobe_ref[k, start : start + CHUNK, :] += roll_take(k, start)

        stage(part_5)

        return found

    def visit(pair, carry):
        last = count_ref[0] - 1
        slots = (2 * pair, jnp.minimum(2 * pair + 1, last))
        valid = (None, 2 * pair + 1 <= last)
        each = [position(s, v, *refs) for s, v, refs in zip(slots, valid, sets)]
        for step in range(len(each[0]) + SKEW):
            if step < len(each[0]):
                each[0][step]()
            if step >= SKEW:
                each[1][step - SKEW]()
        return carry

    lax.fori_loop(0, (count_ref[0] + 1) // 2, visit, 0)


def sort_measured(count, values, order):
    return pl.pallas_call(
        sort_kernel,
        out_shape=jax.ShapeDtypeStruct(values.shape, values.dtype),
        in_specs=[pl.BlockSpec(memory_space=pltpu.SMEM)] + [pl.BlockSpec(memory_space=pltpu.VMEM)] * 2,
        out_specs=pl.BlockSpec(memory_space=pltpu.VMEM),
        compiler_params=pltpu.CompilerParams(vmem_limit_bytes=24 * 1024 * 1024),
        name="sort_measured",
    )(count, values, order)


def call(kernel, name, inputs, scalars, outputs, scratch, size, products):
    f32, bf16 = jnp.float32, jnp.bfloat16
    vmem = pl.BlockSpec(memory_space=pltpu.VMEM)
    work = [pltpu.VMEM((2, size, size), bf16)] * 4 + [pltpu.VMEM((2, size, size), f32)] * 2
    return pl.pallas_call(
        kernel,
        out_shape=[jax.ShapeDtypeStruct(s, f32) for s in outputs],
        in_specs=[pl.BlockSpec(memory_space=pltpu.SMEM)] * scalars + [vmem] * (len(inputs) - scalars),
        out_specs=[vmem] * len(outputs),
        scratch_shapes=([pltpu.VMEM(s, f32) for s in scratch] + work) * 2,
        compiler_params=pltpu.CompilerParams(vmem_limit_bytes=24 * 1024 * 1024),
        cost_estimate=pl.CostEstimate(
            flops=products * 2 * size**3, transcendentals=0, bytes_accessed=sum(x.size * 4 for x in inputs)
        ),
        name=name,
    )(*inputs)


def shifted(value, axis, step):
    count = lax.axis_size(axis)
    return lax.ppermute(value, axis, [(i, (i + step) % count) for i in range(count)])


def pack(value):
    rows = value.shape[1] // 2
    return jnp.concatenate([value[:, :rows], value[:, rows:]], axis=2)


def unpack(from_right, from_left):
    parts_of = [
        jnp.concatenate([from_right[..., s], from_left[..., s]], axis=2)
        for s in (slice(0, MARGIN), slice(MARGIN, None))
    ]
    return jnp.concatenate(parts_of, axis=1)


def swap_cols(to_left, to_right):
    return unpack(shifted(pack(to_left), "tx", -1), shifted(pack(to_right), "tx", 1))


def sides(core):
    size = core.shape[1]
    from_below = shifted(core[:, :MARGIN], "ty", -1)
    from_above = shifted(core[:, size - MARGIN :], "ty", 1)
    col = swap_cols(core[:, :, :MARGIN], core[:, :, size - MARGIN :])
    return jnp.concatenate([from_below, from_above], axis=1), col


def corners(row):
    return swap_cols(row[:, :, :MARGIN], row[:, :, row.shape[2] - MARGIN :])


def owned_cols(side):
    from_left = shifted(pack(side[:, :, :MARGIN]), "tx", 1)
    from_right = shifted(pack(side[:, :, MARGIN:]), "tx", -1)
    return unpack(from_left, from_right)


def owned_rows(side):
    return shifted(side[:, :MARGIN], "ty", 1), shifted(side[:, MARGIN:], "ty", -1)


def spread_cols(side, size):
    gap = jnp.zeros(side.shape[:2] + (size - 2 * MARGIN,), side.dtype)
    return jnp.concatenate([side[:, :, :MARGIN], gap, side[:, :, MARGIN:]], axis=2)


def spread_rows(low, high, size):
    gap = jnp.zeros((low.shape[0], size - 2 * MARGIN, low.shape[2]), low.dtype)
    return jnp.concatenate([low, gap, high], axis=1)


def split(count, inner):
    found = []
    while inner < count:
        members = 4 if (count // inner) % 4 == 0 else 2
        found.append((inner, members))
        inner *= members
    return found


def ring(axis, inner, members, step):
    count = lax.axis_size(axis)
    pairs = []
    for i in range(count):
        low, mid, high = i % inner, (i // inner) % members, i // (inner * members)
        pairs.append((i, (high * members + (mid + step) % members) * inner + low))
    return pairs


def place(axis, inner, members):
    return (lax.axis_index(axis) // inner) % members


def scatter_round(value, axis, inner, members):
    pieces = value.reshape((members, value.shape[0] // members) + value.shape[1:])
    me = place(axis, inner, members)
    pick = lambda step: lax.dynamic_index_in_dim(pieces, (me + step) % members, 0, keepdims=False)
    out = pick(0)
    for got in [lax.ppermute(pick(s), axis, ring(axis, inner, members, s)) for s in range(1, members)]:
        out = out + got
    return out


def gather_round(value, axis, inner, members):
    me = place(axis, inner, members)
    got = [value] + [lax.ppermute(value, axis, ring(axis, inner, members, s)) for s in range(1, members)]
    out = jnp.zeros((members,) + value.shape, value.dtype)
    for step, piece in enumerate(got):
        out = lax.dynamic_update_index_in_dim(out, piece, (me + members - step) % members, 0)
    return out.reshape((members * value.shape[0],) + value.shape[1:])


def exchange_round(value, axis, inner, members):
    out = value
    for got in [lax.ppermute(value, axis, ring(axis, inner, members, s)) for s in range(1, members)]:
        out = out + got
    return out


def total_over_devices(value):
    flat = value.reshape(value.shape[0] * value.shape[1], value.shape[2])
    steps = [("tx", 1, 2)] + [("ty", *s) for s in split(lax.axis_size("ty"), 1)]
    for each in steps:
        flat = scatter_round(flat, *each)
    for each in split(lax.axis_size("tx"), 2):
        flat = exchange_round(flat, "tx", *each)
    for each in reversed(steps):
        flat = gather_round(flat, *each)
    return flat.reshape(value.shape)


def make_body(table, order):
    def body(object_slices, probe, position_count, offsets, intensities):
        size = probe.shape[1]
        devices = lax.axis_size("ty") * lax.axis_size("tx")
        count = position_count.reshape(1)
        place_of = offsets.reshape(offsets.shape[2:])
        core = object_slices.reshape((4,) + object_slices.shape[2:])
        measured = sort_measured(count, intensities.reshape(intensities.shape[2:]), order)
        row, col = sides(core)
        for step in range(ITERS):
            inputs = (count, place_of, core, row, col, corners(row), probe, measured, table)
            plane, field = (2, size, size), (4, size, size)
            gcore, grow, gcol, gcorner, gprobe = call(
                grad_kernel, "gradients", inputs, 2, [x.shape for x in inputs[2:7]],
                [field, plane, plane, (2, size, size)], size, 240,
            )
            peak = jnp.max(probe[0] * probe[0] + probe[1] * probe[1]) + 1e-06
            low, high = owned_rows(grow + spread_cols(owned_cols(gcorner), size))
            total = gcore + spread_cols(owned_cols(gcol), size) + spread_rows(low, high, size)
            core = core - object_rate / peak * total
            summed = total_over_devices(gprobe)
            if step + 1 < ITERS:
                row, col = sides(core)
            probe = probe - probe_rate / devices * summed
        return core.reshape(object_slices.shape), probe

    return body


def solution(mesh):
    size = 256
    table, order = tables(size), lane_order(size)

    def run(object_slices, probe, position_count, offsets, intensities):
        placed = (
            P(None, None, "ty", "tx"),
            P(),
            P("ty", "tx"),
            P("ty", "tx", None, None),
            P("ty", "tx", None, None, None),
        )
        return jax.shard_map(
            make_body(jnp.asarray(table), jnp.asarray(order)),
            mesh=mesh,
            in_specs=placed,
            out_specs=(P(None, None, "ty", "tx"), P()),
            check_vma=False,
        )(object_slices, probe, position_count, offsets, intensities)

    return run
```

```python
import math

import jax
import jax.numpy as jnp
import ml_dtypes
import numpy as np
from jax import lax
from jax.experimental import pallas as pl
from jax.experimental.pallas import tpu as pltpu
from jax.sharding import PartitionSpec as P

MARGIN = 64
ITERS = 2
CHUNK = 16
SKEW = 0

chirp_rate = 0.5
object_rate = 0.5
probe_rate = 2.0


def tables(size):
    index = np.arange(size)
    four = np.exp(-2j * np.pi * (np.outer(index, index) % size) / size) / math.sqrt(size)
    centred = (index + size // 2) % size - size // 2
    kernel = np.exp(-1j * chirp_rate * np.pi * centred * centred / size)
    prop = (four.conj() * kernel[None, :]) @ four
    half = size // 2
    near, far = prop[:half, :half], prop[:half, half:]
    blocks = ((0.5 * (near + far), 0.5 * (near - far)), (four[0::2, :half], four[1::2, :half]))
    out = np.zeros((2, 2, 2, 2, size, size), ml_dtypes.bfloat16)
    for family in range(2):
        for parity in range(2):
            block = blocks[family][parity]
            left = np.block([[block.real, -block.imag], [block.imag, block.real]])
            for form, value in enumerate((left, left.T)):
                high = value.astype(np.float32).astype(ml_dtypes.bfloat16)
                low = (value - high.astype(np.float64)).astype(np.float32).astype(ml_dtypes.bfloat16)
                out[family, parity, form, 0] = high
                out[family, parity, form, 1] = low
    return out


def lane_order(size):
    out = np.zeros((size, size), ml_dtypes.bfloat16)
    half = size // 2
    for lane in range(half):
        out[2 * lane, lane] = 1
        out[2 * lane + 1, half + lane] = 1
    return np.stack([out, out.T])


def dot(left, right):
    return jnp.dot(left, right, preferred_element_type=jnp.float32)


def parts(value):
    high = value.astype(jnp.bfloat16)
    low = (value - high.astype(jnp.float32)).astype(jnp.bfloat16)
    return high, low


def thirds(value):
    first = value.astype(jnp.bfloat16)
    rest = value - first.astype(jnp.float32)
    second = rest.astype(jnp.bfloat16)
    return first, second, (rest - second.astype(jnp.float32)).astype(jnp.bfloat16)


def sort_kernel(count_ref, values_ref, order_ref, out_ref):
    out_ref[...] = jnp.zeros_like(out_ref)

    def visit(slot, carry):
        first, second, third = [dot(x, order_ref[0]) for x in thirds(values_ref[slot])]
        first, second, third = [dot(order_ref[1], x) for x in thirds((first + second) + third)]
        out_ref[slot] = (first + second) + third
        return carry

    lax.fori_loop(0, count_ref[0], visit, 0)


def common(size):
    half, quarter = size // 2, size // 4

    def at(part, start):
        return pl.ds(part * half + start, CHUNK)

    def lanes(part):
        return pl.ds(part * half, half)

    def boundary(part, start):
        return (start < quarter) == (part == 0)

    return half, at, lanes, boundary


def fold(quads):
    mixed = [[quads[0][c] + quads[1][c] for c in range(2)], [quads[0][c] - quads[1][c] for c in range(2)]]
    return [[m[0] + m[1], m[0] - m[1]] for m in mixed]


def empty():
    return [[None, None], [None, None]]


def masks(size, top, lead):
    half = size // 2
    lane = lax.broadcasted_iota(jnp.int32, (CHUNK, half), 1)
    row = lax.broadcasted_iota(jnp.int32, (CHUNK, half), 0)
    cols = (lane + MARGIN >= lead, lane - MARGIN < lead)

    def row_mask(part, start):
        inside = row + start
        return inside + MARGIN >= top if part == 0 else inside - MARGIN < top

    return cols, row_mask


def stages(size, table_ref, high_ref, low_ref, rhigh_ref, rlow_ref, mid_ref, back_ref):
    half, at, lanes, _ = common(size)

    def put(start, real, imag):
        for p in range(2):
            for q in range(2):
                for comp, value in ((0, real[p][q]), (1, imag[p][q])):
                    high, low = parts(value)
                    high_ref[q, at(p, start), lanes(comp)] = high
                    low_ref[q, at(p, start), lanes(comp)] = low

    def right(family, form):
        for q in range(2):
            weight, small = table_ref[family, q, form, 0], table_ref[family, q, form, 1]
            mid_ref[q] = dot(high_ref[q], weight) + dot(low_ref[q], weight) + dot(high_ref[q], small)
        for q in range(2):
            for p in range(2):
                for start in range(0, half, CHUNK):
                    for comp in range(2):
                        high, low = parts(mid_ref[q, at(p, start), lanes(comp)])
                        rhigh_ref[p, at(comp, start), lanes(q)] = high
                        rlow_ref[p, at(comp, start), lanes(q)] = low

    def left(family, form):
        for p in range(2):
            weight, small = table_ref[family, p, 1 - form, 0], table_ref[family, p, 1 - form, 1]
            back_ref[p] = dot(weight, rhigh_ref[p]) + dot(small, rhigh_ref[p]) + dot(weight, rlow_ref[p])

    def take(start, comp):
        return [[back_ref[p, at(comp, start), lanes(q)] for q in range(2)] for p in range(2)]

    return put, right, left, take


def window_of(size, core_ref, row_ref, col_ref, corner_ref, cols, row_mask):
    half, at, lanes, boundary = common(size)

    def window(start, k):
        out = empty()
        for r in range(2):
            other = col_ref[k, at(r, start), :]
            if boundary(r, start):
                mask = row_mask(r, start)
                other = jnp.where(mask, other, corner_ref[k, pl.ds(start, CHUNK), :])
            for c in range(2):
                own = core_ref[k, at(r, start), lanes(c)]
                if boundary(r, start):
                    own = jnp.where(mask, own, row_ref[k, pl.ds(start, CHUNK), lanes(c)])
                out[r][c] = jnp.where(cols[c], own, other)
        return out

    return window


def collect_into(size, gcore_ref, grow_ref, gcol_ref, gcorner_ref, cols, row_mask):
    half, at, lanes, boundary = common(size)

    def collect(start, k, quads):
        for r in range(2):
            side = jnp.where(cols[0], jnp.where(cols[1], 0.0, quads[r][1]), quads[r][0])
            own = [jnp.where(cols[c], quads[r][c], 0.0) for c in range(2)]
            if boundary(r, start):
                mask = row_mask(r, start)
                for c in range(2):
                    gcore_ref[k, at(r, start), lanes(c)] += jnp.where(mask, own[c], 0.0)
                    grow_ref[k, pl.ds(start, CHUNK), lanes(c)] += jnp.where(mask, 0.0, own[c])
                gcol_ref[k, at(r, start), :] += jnp.where(mask, side, 0.0)
                gcorner_ref[k, pl.ds(start, CHUNK), :] += jnp.where(mask, 0.0, side)
            else:
                for c in range(2):
                    gcore_ref[k, at(r, start), lanes(c)] += own[c]
                gcol_ref[k, at(r, start), :] += side

    return collect


TILE = 8


def roller(size, shift_row, shift_col, twice_ref):
    half = size // 2
    lane = lax.broadcasted_iota(jnp.int32, (TILE, half), 1)
    far = (shift_col >= half).astype(jnp.int32)
    step = shift_col - far * half
    other = (lane < step).astype(jnp.int32) != far
    whole = shift_row // TILE
    rest = shift_row - whole * TILE
    row = lax.broadcasted_iota(jnp.int32, (CHUNK, size), 0)
    early = lax.rem(row, TILE) < rest

    def put(k, start, low, high):
        low, high = pltpu.roll(low, step, 1), pltpu.roll(high, step, 1)
        turned = (jnp.where(other, high, low), jnp.where(other, low, high))
        for c in range(2):
            value = pltpu.roll(turned[c], rest, 0)
            twice_ref[k, start : start + TILE, c * half : (c + 1) * half] = value

    def take(k, start):
        tiles = [
            pl.multiple_of(lax.rem(size + start + step * TILE - whole * TILE, size), TILE)
            for step in range(-1, CHUNK // TILE)
        ]
        rows = jnp.concatenate([twice_ref[k, pl.ds(tile, TILE), :] for tile in tiles], axis=0)
        return jnp.where(early, rows[:CHUNK], rows[TILE:])

    return put, take


def shifts(size, top, lead):
    return lax.rem(top + (size - MARGIN), size), lax.rem(lead + (size - MARGIN), size)


def grad_kernel(
    count_ref, offset_ref, core_ref, row_ref, col_ref, corner_ref, probe_ref, measured_ref, table_ref,
    gcore_ref, grow_ref, gcol_ref, gcorner_ref, gprobe_ref, *scratch,
):
    size = probe_ref.shape[1]
    half, at, lanes, _ = common(size)
    sets = [scratch[: len(scratch) // 2], scratch[len(scratch) // 2 :]]
    for ref in (gcore_ref, grow_ref, gcol_ref, gcorner_ref, gprobe_ref):
        ref[...] = jnp.zeros_like(ref)

    def position(slot, valid, window_ref, moved_ref, rolled_ref, twice_ref, *work):
        put, right, left, take = stages(size, table_ref, *work)
        found = []
        stage = found.append
        top, lead = offset_ref[slot, 0], offset_ref[slot, 1]
        shift_row, shift_col = shifts(size, top, lead)
        cols, row_mask = masks(size, top, lead)
        window = window_of(size, core_ref, row_ref, col_ref, corner_ref, cols, row_mask)
        collect = collect_into(size, gcore_ref, grow_ref, gcol_ref, gcorner_ref, cols, row_mask)
        roll_put, roll_take = roller(size, shift_row, shift_col, twice_ref)

        def part_1():
            for k in range(2):
                for start in range(0, size, TILE):
                    roll_put(k, start, *[probe_ref[k, pl.ds(start, TILE), lanes(c)] for c in range(2)])
            for start in range(0, half, CHUNK):
                one_real, one_imag = window(start, 0), window(start, 1)
                real, imag = empty(), empty()
                for r in range(2):
                    turned = [roll_take(k, r * half + start) for k in range(2)]
                    for c in range(2):
                        pr, pi = [t[:, c * half : (c + 1) * half] for t in turned]
                        wr, wi = one_real[r][c], one_imag[r][c]
                        rolled_ref[0, at(r, start), lanes(c)] = pr
                        rolled_ref[1, at(r, start), lanes(c)] = pi
                        window_ref[0, at(r, start), lanes(c)] = wr
                        window_ref[1, at(r, start), lanes(c)] = wi
                        real[r][c] = pr * wr - pi * wi
                        imag[r][c] = pr * wi + pi * wr
                put(start, fold(real), fold(imag))
        stage(part_1)

        stage(lambda: right(0, 1))
        stage(lambda: left(0, 1))
        def part_2():
            for start in range(0, half, CHUNK):
                moved_real, moved_imag = fold(take(start, 0)), fold(take(start, 1))
                two_real, two_imag = window(start, 2), window(start, 3)
                real, imag = empty(), empty()
                for r in range(2):
                    for c in range(2):
                        mr, mi = moved_real[r][c], moved_imag[r][c]
                        tr, ti = two_real[r][c], two_imag[r][c]
                        moved_ref[0, at(r, start), lanes(c)] = mr
                        moved_ref[1, at(r, start), lanes(c)] = mi
                        window_ref[2, at(r, start), lanes(c)] = tr
                        window_ref[3, at(r, start), lanes(c)] = ti
                        real[r][c] = mr * tr - mi * ti
                        imag[r][c] = mr * ti + mi * tr
                put(start, fold(real), fold(imag))
        stage(part_2)

        stage(lambda: right(1, 1))
        stage(lambda: left(1, 1))
        def part_3():
            for start in range(0, half, CHUNK):
                far_real, far_imag = take(start, 0), take(start, 1)
                real, imag = empty(), empty()
                for p in range(2):
                    for q in range(2):
                        fr, fi = far_real[p][q], far_imag[p][q]
                        misfit = fr * fr + fi * fi - measured_ref[slot, at(p, start), lanes(q)]
                        if valid is not None:
                            misfit = jnp.where(valid, misfit, 0.0)
                        real[p][q] = misfit * fr
                        imag[p][q] = misfit * fi
                put(start, real, imag)
        stage(part_3)

        stage(lambda: right(1, 0))
        stage(lambda: left(1, 0))
        def part_4():
            for start in range(0, half, CHUNK):
                back_real, back_imag = fold(take(start, 0)), fold(take(start, 1))
                real, imag, two_real, two_imag = empty(), empty(), empty(), empty()
                for r in range(2):
                    for c in range(2):
                        br, bi = back_real[r][c], back_imag[r][c]
                        mr, mi = [moved_ref[k, at(r, start), lanes(c)] for k in range(2)]
                        tr, ti = [window_ref[k, at(r, start), lanes(c)] for k in (2, 3)]
                        two_real[r][c] = mr * br + mi * bi
                        two_imag[r][c] = mr * bi - mi * br
                        real[r][c] = tr * br + ti * bi
                        imag[r][c] = tr * bi - ti * br
                put(start, fold(real), fold(imag))
                collect(start, 2, two_real)
                collect(start, 3, two_imag)
        stage(part_4)

        stage(lambda: right(0, 0))
        stage(lambda: left(0, 0))
        def part_5():
            roll_put, roll_take = roller(
                size, lax.rem(size - shift_row, size), lax.rem(size - shift_col, size), twice_ref
            )
            for start in range(0, half, CHUNK):
                wave_real, wave_imag = fold(take(start, 0)), fold(take(start, 1))
                one_real, one_imag = empty(), empty()
                for r in range(2):
                    turned = empty()
                    for c in range(2):
                        wr, wi = wave_real[r][c], wave_imag[r][c]
                        pr, pi = [rolled_ref[k, at(r, start), lanes(c)] for k in range(2)]
                        fr, fi = [window_ref[k, at(r, start), lanes(c)] for k in range(2)]
                        one_real[r][c] = pr * wr + pi * wi
                        one_imag[r][c] = pr * wi - pi * wr
                        turned[0][c] = fr * wr + fi * wi
                        turned[1][c] = fr * wi - fi * wr
                    for k in range(2):
                        for tile in range(0, CHUNK, TILE):
                            roll_put(k, r * half + start + tile, *[t[tile : tile + TILE] for t in turned[k]])
                collect(start, 0, one_real)
                collect(start, 1, one_imag)
            for k in range(2):
                for start in range(0, size, CHUNK):
                    gprobe_ref[k, start : start + CHUNK, :] += roll_take(k, start)

        stage(part_5)

        return found

    def visit(pair, carry):
        last = count_ref[0] - 1
        slots = (2 * pair, jnp.minimum(2 * pair + 1, last))
        valid = (None, 2 * pair + 1 <= last)
        each = [position(s, v, *refs) for s, v, refs in zip(slots, valid, sets)]
        for step in range(len(each[0]) + SKEW):
            if step < len(each[0]):
                each[0][step]()
            if step >= SKEW:
                each[1][step - SKEW]()
        return carry

    lax.fori_loop(0, (count_ref[0] + 1) // 2, visit, 0)


def sort_measured(count, values, order):
    return pl.pallas_call(
        sort_kernel,
        out_shape=jax.ShapeDtypeStruct(values.shape, values.dtype),
        in_specs=[pl.BlockSpec(memory_space=pltpu.SMEM)] + [pl.BlockSpec(memory_space=pltpu.VMEM)] * 2,
        out_specs=pl.BlockSpec(memory_space=pltpu.VMEM),
        compiler_params=pltpu.CompilerParams(vmem_limit_bytes=24 * 1024 * 1024),
        name="sort_measured",
    )(count, values, order)


def call(kernel, name, inputs, scalars, outputs, scratch, size, products):
    f32, bf16 = jnp.float32, jnp.bfloat16
    vmem = pl.BlockSpec(memory_space=pltpu.VMEM)
    work = [pltpu.VMEM((2, size, size), bf16)] * 4 + [pltpu.VMEM((2, size, size), f32)] * 2
    return pl.pallas_call(
        kernel,
        out_shape=[jax.ShapeDtypeStruct(s, f32) for s in outputs],
        in_specs=[pl.BlockSpec(memory_space=pltpu.SMEM)] * scalars + [vmem] * (len(inputs) - scalars),
        out_specs=[vmem] * len(outputs),
        scratch_shapes=([pltpu.VMEM(s, f32) for s in scratch] + work) * 2,
        compiler_params=pltpu.CompilerParams(vmem_limit_bytes=24 * 1024 * 1024),
        cost_estimate=pl.CostEstimate(
            flops=products * 2 * size**3, transcendentals=0, bytes_accessed=sum(x.size * 4 for x in inputs)
        ),
        name=name,
    )(*inputs)


def shifted(value, axis, step):
    count = lax.axis_size(axis)
    return lax.ppermute(value, axis, [(i, (i + step) % count) for i in range(count)])


def pack(value):
    rows = value.shape[1] // 2
    return jnp.concatenate([value[:, :rows], value[:, rows:]], axis=2)


def unpack(from_right, from_left):
    parts_of = [
        jnp.concatenate([from_right[..., s], from_left[..., s]], axis=2)
        for s in (slice(0, MARGIN), slice(MARGIN, None))
    ]
    return jnp.concatenate(parts_of, axis=1)


def swap_cols(to_left, to_right):
    return unpack(shifted(pack(to_left), "tx", -1), shifted(pack(to_right), "tx", 1))


def sides(core):
    size = core.shape[1]
    from_below = shifted(core[:, :MARGIN], "ty", -1)
    from_above = shifted(core[:, size - MARGIN :], "ty", 1)
    col = swap_cols(core[:, :, :MARGIN], core[:, :, size - MARGIN :])
    return jnp.concatenate([from_below, from_above], axis=1), col


def corners(row):
    return swap_cols(row[:, :, :MARGIN], row[:, :, row.shape[2] - MARGIN :])


def owned_cols(side):
    from_left = shifted(pack(side[:, :, :MARGIN]), "tx", 1)
    from_right = shifted(pack(side[:, :, MARGIN:]), "tx", -1)
    return unpack(from_left, from_right)


def owned_rows(side):
    return shifted(side[:, :MARGIN], "ty", 1), shifted(side[:, MARGIN:], "ty", -1)


def spread_cols(side, size):
    gap = jnp.zeros(side.shape[:2] + (size - 2 * MARGIN,), side.dtype)
    return jnp.concatenate([side[:, :, :MARGIN], gap, side[:, :, MARGIN:]], axis=2)


def spread_rows(low, high, size):
    gap = jnp.zeros((low.shape[0], size - 2 * MARGIN, low.shape[2]), low.dtype)
    return jnp.concatenate([low, gap, high], axis=1)


def split(count, inner):
    found = []
    while inner < count:
        members = 4 if (count // inner) % 4 == 0 else 2
        found.append((inner, members))
        inner *= members
    return found


def ring(axis, inner, members, step):
    count = lax.axis_size(axis)
    pairs = []
    for i in range(count):
        low, mid, high = i % inner, (i // inner) % members, i // (inner * members)
        pairs.append((i, (high * members + (mid + step) % members) * inner + low))
    return pairs


def place(axis, inner, members):
    return (lax.axis_index(axis) // inner) % members


def scatter_round(value, axis, inner, members):
    pieces = value.reshape((members, value.shape[0] // members) + value.shape[1:])
    me = place(axis, inner, members)
    pick = lambda step: lax.dynamic_index_in_dim(pieces, (me + step) % members, 0, keepdims=False)
    out = pick(0)
    for got in [lax.ppermute(pick(s), axis, ring(axis, inner, members, s)) for s in range(1, members)]:
        out = out + got
    return out


def gather_round(value, axis, inner, members):
    me = place(axis, inner, members)
    got = [value] + [lax.ppermute(value, axis, ring(axis, inner, members, s)) for s in range(1, members)]
    out = jnp.zeros((members,) + value.shape, value.dtype)
    for step, piece in enumerate(got):
        out = lax.dynamic_update_index_in_dim(out, piece, (me + members - step) % members, 0)
    return out.reshape((members * value.shape[0],) + value.shape[1:])


def exchange_round(value, axis, inner, members):
    out = value
    for got in [lax.ppermute(value, axis, ring(axis, inner, members, s)) for s in range(1, members)]:
        out = out + got
    return out


def total_over_devices(value):
    flat = value.reshape(value.shape[0] * value.shape[1], value.shape[2])
    steps = [("tx", 1, 2)] + [("ty", *s) for s in split(lax.axis_size("ty"), 1)]
    for each in steps:
        flat = scatter_round(flat, *each)
    for each in split(lax.axis_size("tx"), 2):
        flat = exchange_round(flat, "tx", *each)
    for each in reversed(steps):
        flat = gather_round(flat, *each)
    return flat.reshape(value.shape)


def make_body(table, order):
    def body(object_slices, probe, position_count, offsets, intensities):
        size = probe.shape[1]
        devices = lax.axis_size("ty") * lax.axis_size("tx")
        count = position_count.reshape(1)
        place_of = offsets.reshape(offsets.shape[2:])
        core = object_slices.reshape((4,) + object_slices.shape[2:])
        measured = sort_measured(count, intensities.reshape(intensities.shape[2:]), order)
        row, col = sides(core)
        for step in range(ITERS):
            inputs = (count, place_of, core, row, col, corners(row), probe, measured, table)
            plane, field = (2, size, size), (4, size, size)
            gcore, grow, gcol, gcorner, gprobe = call(
                grad_kernel, "gradients", inputs, 2, [x.shape for x in inputs[2:7]],
                [field, plane, plane, (2, size, size)], size, 240,
            )
            peak = jnp.max(probe[0] * probe[0] + probe[1] * probe[1]) + 1e-06
            owned = owned_cols(jnp.concatenate([gcol, gcorner], axis=1))
            low, high = owned_rows(grow + spread_cols(owned[:, size:], size))
            total = gcore + spread_cols(owned[:, :size], size) + spread_rows(low, high, size)
            core = core - object_rate / peak * total
            summed = total_over_devices(gprobe)
            if step + 1 < ITERS:
                row, col = sides(core)
            probe = probe - probe_rate / devices * summed
        return core.reshape(object_slices.shape), probe

    return body


def solution(mesh):
    size = 256
    table, order = tables(size), lane_order(size)

    def run(object_slices, probe, position_count, offsets, intensities):
        placed = (
            P(None, None, "ty", "tx"),
            P(),
            P("ty", "tx"),
            P("ty", "tx", None, None),
            P("ty", "tx", None, None, None),
        )
        return jax.shard_map(
            make_body(jnp.asarray(table), jnp.asarray(order)),
            mesh=mesh,
            in_specs=placed,
            out_specs=(P(None, None, "ty", "tx"), P()),
            check_vma=False,
        )(object_slices, probe, position_count, offsets, intensities)

    return run
```
